256 devices in a mesh: section: 8 (over x, core), sp: 32 (over y, z).
Axes of the slice: x: 4, y: 4, z: 8, core: 2. Of those that a mesh axis runs over, the one named last changes fastest.
Arguments:
- field_in: bfloat16 [8, 384, 192, 768], P('section', 'sp'), may hold values from -6 to 6
- spectral_gain: bfloat16 [8, 192], P('section'), may hold values from 0.5 to 1.5
- spectral_weight: bfloat16 [8, 384, 192, 384], P('section', 'sp'), may hold values from -0.3125 to 0.3125
- mixer_gain: bfloat16 [8, 192], P('section'), may hold values from 0.5 to 1.5
- up_weight: bfloat16 [8, 192, 384], P('section'), may hold values from -0.4375 to 0.4375
- up_bias: bfloat16 [8, 384], P('section'), may hold values from -3 to 3
- down_weight: bfloat16 [8, 192, 384], P('section'), may hold values from -0.3125 to 0.3125
Outputs:
- next_field: bfloat16 [8, 384, 192, 768], P('section', 'sp')
The draws below stay inside these ranges and needn't reach their ends.
All inputs are finite; a program needn't handle non-finite values.
Results may differ from the reference program's by a relative error of at most 0.012.
Values may be sent and summed in bfloat16 or wider, within the bound.
No kernel may reach another device: no remote copies, remote signals or barrier semaphores. Data moves between devices by JAX's collectives and lax.ppermute only.
A program may use at most 128 MiB of HBM per device.

```python
import math
import jax
import jax.numpy as jnp
from jax import lax

C = 192
HID = 384
NLAT = 384
NLON = 768
LMAX = 384
MMAX = 384
SECTIONS = 8


def shard_levels(rng, extent, split, smallest, top_value):
    def one(dim, shards_of):
        draws = jax.random.uniform(jax.random.fold_in(jax.random.fold_in(rng, 6), dim), (shards_of,), jnp.float32, smallest / len(split), top_value / len(split))
        return jnp.repeat(jnp.exp(draws), extent[dim] // shards_of).reshape((-1,) + (1,) * (len(extent) - dim - 1))

    level = one(*split[0])
    for cut in split[1:]:
        level = level * one(*cut)
    return level


def scatter_about(rng, dims, scale, most, pieces=(), kind=jnp.bfloat16):
    values = jax.random.normal(rng, dims, jnp.float32) * scale
    if len(pieces) > 0:
        values = shard_levels(rng, dims, pieces, -0.22, 0.18) * values
    return jnp.clip(values, min=-most, max=most).astype(kind)


def setup_inputs(seed: int = 0) -> dict:
    streams_of = jax.random.split(jax.random.key(seed), 8)
    return {
        "field_in": scatter_about(streams_of[0], (SECTIONS, NLAT, C, NLON), 1.0, 6.0, ((0, 8), (1, 32))),
        "spectral_gain": jnp.clip(1.0 + 0.1 * jax.random.normal(streams_of[1], (SECTIONS, C), jnp.float32), 0.5, 1.5).astype(jnp.bfloat16),
        "spectral_weight": scatter_about(streams_of[2], (SECTIONS, LMAX, C, 2 * C), (2 * C) ** -0.5, 0.3125, ((0, 8), (1, 32))),
        "mixer_gain": jnp.clip(1.0 + 0.1 * jax.random.normal(streams_of[3], (SECTIONS, C), jnp.float32), 0.5, 1.5).astype(jnp.bfloat16),
        "up_weight": scatter_about(streams_of[4], (SECTIONS, C, HID), C ** -0.5, 0.4375, ((0, 8),)),
        "up_bias": scatter_about(streams_of[5], (SECTIONS, HID), 0.5, 3.0, ((0, 8),)),
        "down_weight": scatter_about(streams_of[6], (SECTIONS, C, HID), HID ** -0.5, 0.3125, ((0, 8),)),
    }


EPSILON = 1e-05

def quad_weights(cycle_index, cycle_count):
    terms_count = cycle_count // 2
    orders = jnp.arange(1, terms_count + 1, dtype=jnp.int32)
    phase_turns = orders[None, :] * (2 * cycle_index[:, None] + 1) % (2 * cycle_count)
    angles = math.pi * phase_turns.astype(jnp.float32) / cycle_count
    orders_real = orders.astype(jnp.float32)
    series = lax.optimization_barrier(jnp.sum(jnp.cos(angles) / (4.0 * orders_real * orders_real - 1.0)[None, :], axis=1))
    return 2.0 / cycle_count * (1.0 - 2.0 * series)

def fourier_tables(point_count, orders):
    points = jnp.arange(point_count, dtype=jnp.int32)
    phase_turns = points[:, None] * orders[None, :] % point_count
    angles = 2.0 * math.pi / point_count * phase_turns.astype(jnp.float32)
    cosines = jnp.cos(angles)
    sine_values = jnp.sin(angles)
    forward = jnp.stack([cosines, -sine_values], axis=1).astype(jnp.bfloat16)
    doubling = jnp.where(orders == 0, 1.0, 2.0).astype(jnp.float32)[:, None]
    inverse = jnp.stack([cosines.T * doubling, -sine_values.T * doubling], axis=0).astype(jnp.bfloat16)
    return (forward, inverse)

def step_entries(degree, order_col, cosines):
    active = degree >= order_col + 1.0
    further = degree >= order_col + 2.0
    degree_sq = degree * degree
    order_sq = order_col * order_col
    lead_coeff = jnp.sqrt(jnp.where(active, (4.0 * degree_sq - 1.0) / jnp.where(active, degree_sq - order_sq, 1.0), 0.0))
    before = degree - 1.0
    before_sq = before * before
    trail_coeff = jnp.sqrt(jnp.where(further, (before_sq - order_sq) / jnp.where(further, 4.0 * before_sq - 1.0, 1.0), 0.0))
    diag_top = jnp.where(active, lead_coeff * cosines, 1.0)
    off_top = jnp.where(active, -lead_coeff * trail_coeff, 0.0)
    off_low = jnp.where(active, 1.0, 0.0)
    diag_low = jnp.where(active, 0.0, 1.0)
    return (diag_top, off_top, off_low, diag_low)

def legendre_rows(order_index, cycle_count, degree_count):
    colatitude = math.pi * (jnp.arange(cycle_count, dtype=jnp.float32) + 0.5) / cycle_count
    cosines = jnp.cos(colatitude)[None, None, :]
    sine_values = jnp.sin(colatitude)
    order_real = order_index.astype(jnp.float32)
    steps_all = jnp.arange(1, degree_count + 1, dtype=jnp.float32)
    factors = jnp.log((2.0 * steps_all - 1.0) / (2.0 * steps_all))
    below_mask = (steps_all[None, :] <= order_real[:, None]).astype(jnp.float32)
    partial_log = lax.optimization_barrier(jnp.sum(below_mask * factors[None, :], axis=1))
    start_log = 0.5 * jnp.log((2.0 * order_real + 1.0) / (4.0 * math.pi)) + 0.5 * partial_log
    start_log = start_log[:, None] + order_real[:, None] * jnp.log(sine_values)[None, :]
    order_col = order_real[None, :, None]
    block_count = degree_count // 16
    block_base = (16 * jnp.arange(block_count, dtype=jnp.int32)).astype(jnp.float32)[:, None, None]
    shape_all = (block_count, order_index.shape[0], cycle_count)
    unit_array = jnp.ones(shape_all, jnp.float32)
    zero_array = jnp.zeros(shape_all, jnp.float32)

    def product_half(half_turn, matrices):
        upper_left, upper_right, lower_left, lower_right, log_scale = matrices
        for inner_step in range(8):
            degree = block_base + (half_turn * 8 + inner_step).astype(jnp.float32)
            diag_top, off_top, off_low, diag_low = step_entries(degree, order_col, cosines)
            next_ul = diag_top * upper_left + off_top * lower_left
            next_ur = diag_top * upper_right + off_top * lower_right
            next_ll = off_low * upper_left + diag_low * lower_left
            next_lr = off_low * upper_right + diag_low * lower_right
            largest = jnp.maximum(jnp.maximum(jnp.abs(next_ul), jnp.abs(next_ur)), jnp.maximum(jnp.abs(next_ll), jnp.abs(next_lr)))
            upper_left = next_ul / largest
            upper_right = next_ur / largest
            lower_left = next_ll / largest
            lower_right = next_lr / largest
            log_scale = log_scale + jnp.log(largest)
        return (upper_left, upper_right, lower_left, lower_right, log_scale)
    products = lax.fori_loop(0, 2, product_half, (unit_array, zero_array, zero_array, unit_array, zero_array))

    def carry_block(vector_state, block_matrix):
        lead_value, lag_value, log_value = vector_state
        upper_left, upper_right, lower_left, lower_right, log_scale = block_matrix
        next_lead = upper_left * lead_value + upper_right * lag_value
        next_lag = lower_left * lead_value + lower_right * lag_value
        largest = jnp.maximum(jnp.abs(next_lead), jnp.abs(next_lag))
        return ((next_lead / largest, next_lag / largest, log_value + log_scale + jnp.log(largest)), vector_state)
    initial = (unit_array[0], zero_array[0], start_log)
    final_state, starts = lax.scan(carry_block, initial, products)

    def degree_half(vector_state, half_turn):
        lead_value, lag_value, log_value = vector_state
        values = []
        for inner_step in range(8):
            degree = block_base + (half_turn * 8 + inner_step).astype(jnp.float32)
            diag_top, off_top, off_low, diag_low = step_entries(degree, order_col, cosines)
            next_lead = diag_top * lead_value + off_top * lag_value
            next_lag = off_low * lead_value + diag_low * lag_value
            largest = jnp.maximum(jnp.abs(next_lead), jnp.abs(next_lag))
            lead_value = next_lead / largest
            lag_value = next_lag / largest
            log_value = log_value + jnp.log(largest)
            values.append(lead_value * jnp.exp(log_value))
        return ((lead_value, lag_value, log_value), jnp.stack(values))
    last_state, table_rows = lax.scan(degree_half, starts, jnp.arange(2, dtype=jnp.int32))
    legendre = jnp.transpose(table_rows, (3, 2, 0, 1, 4)).reshape(order_index.shape[0], degree_count, cycle_count)
    degrees = jnp.arange(degree_count, dtype=jnp.int32)
    return jnp.where(degrees[None, :, None] >= order_index[:, None, None], legendre, 0.0)

def layer_norm(values, gain_row):
    values = values.astype(jnp.float32)
    average = lax.optimization_barrier(jnp.mean(values, axis=-2, keepdims=True))
    centred = values - average
    variance = lax.optimization_barrier(jnp.mean(centred * centred, axis=-2, keepdims=True))
    return centred * lax.rsqrt(variance + EPSILON) * gain_row.astype(jnp.float32)[:, None]

def mixing_matrix(weight):
    width = weight.shape[1]
    real_weight = weight[:, :, :width]
    imag_weight = weight[:, :, width:]
    top_half = jnp.concatenate([real_weight, imag_weight], axis=2)
    bottom_half = jnp.concatenate([-imag_weight, real_weight], axis=2)
    return jnp.concatenate([top_half, bottom_half], axis=1)

def section_block(grid_values, spectral_row, weight, mixer_row, up_matrix, bias_row, down_matrix, legendre, forward, inverse, cycle_weight):
    normed = layer_norm(grid_values, spectral_row).astype(jnp.bfloat16)
    spectral = jnp.einsum('nrm,acn->marc', forward.astype(jnp.float32), normed.astype(jnp.float32))
    spectral = (spectral * cycle_weight[None, :, None, None]).astype(jnp.bfloat16).reshape(MMAX, NLAT, 2 * C)
    legendre_real = legendre.astype(jnp.float32)
    coeffs = jnp.einsum('mla,mak->mlk', legendre_real, spectral.astype(jnp.float32)).astype(jnp.bfloat16)
    block_weight = mixing_matrix(weight)
    mixed = jnp.einsum('mlk,lkj->mlj', coeffs.astype(jnp.float32), block_weight.astype(jnp.float32)).astype(jnp.bfloat16)
    grid_part = jnp.einsum('mla,mlk->mak', legendre_real, mixed.astype(jnp.float32)).astype(jnp.bfloat16)
    synthesis = jnp.einsum('marc,rmn->acn', grid_part.reshape(MMAX, NLAT, 2, C).astype(jnp.float32), inverse.astype(jnp.float32))
    residual = grid_values.astype(jnp.float32) + synthesis
    hidden_in = layer_norm(residual, mixer_row).astype(jnp.bfloat16)
    hidden = jnp.einsum('acn,ch->anh', hidden_in.astype(jnp.float32), up_matrix.astype(jnp.float32)) + bias_row.astype(jnp.float32)
    hidden = jax.nn.gelu(hidden, approximate=False).astype(jnp.bfloat16)
    branch = jnp.einsum('anh,ch->acn', hidden.astype(jnp.float32), down_matrix.astype(jnp.float32))
    return (residual + branch).astype(jnp.bfloat16)

def reference(field_in, spectral_gain, spectral_weight, mixer_gain, up_weight, up_bias, down_weight):
    all_orders = jnp.arange(MMAX, dtype=jnp.int32)
    legendre = legendre_rows(all_orders, NLAT, LMAX).astype(jnp.bfloat16)
    forward, inverse = fourier_tables(NLON, all_orders)
    cycle_weight = quad_weights(jnp.arange(NLAT, dtype=jnp.int32), NLAT) * (2.0 * math.pi / NLON)

    def one_section(section_args):
        grid_values, spectral_row, weight, mixer_row, up_matrix, bias_row, down_matrix = section_args
        return section_block(grid_values, spectral_row, weight, mixer_row, up_matrix, bias_row, down_matrix, legendre, forward, inverse, cycle_weight)
    outputs = lax.map(one_section, (field_in, spectral_gain, spectral_weight, mixer_gain, up_weight, up_bias, down_weight))
    return jnp.roll(outputs, 1, axis=0)
```

```python
import math

import jax
import jax.numpy as jnp
from jax import lax
from jax.experimental import pallas as pl
from jax.experimental.pallas import tpu as pltpu
from jax.sharding import PartitionSpec as P


C = 192
HID = 384
NLAT = 384
NLON = 768
LMAX = 384
MMAX = 384
SP = 32
ROWS = NLAT // SP
PAIRS = LMAX // SP // 2
K2 = 2 * C
BLOCK_M = 2 * PAIRS * ROWS
BLOCK_L = 2 * PAIRS * PAIRS
T_ROWS = LMAX
T_PAD = T_ROWS + 8
LANES = 2 * NLAT

EPSILON = 1e-05
SCALE_LOG2 = 64.0
DOWN = 2.0**-64
LIMIT = 2.0**32

F32 = jnp.float32
BF16 = jnp.bfloat16


def pair_low(pair):
    return jnp.minimum(2 * pair, LMAX - 1 - 2 * pair)


def pair_high(pair):
    return jnp.maximum(2 * pair, LMAX - 1 - 2 * pair)


def params(mebibytes):
    return pltpu.CompilerParams(vmem_limit_bytes=mebibytes * 1024 * 1024)


def whole(shape):
    return pl.BlockSpec(shape, lambda *_: (0,) * len(shape))


def quad_weights(cycle_index, cycle_count):
    terms_count = cycle_count // 2
    orders = jnp.arange(1, terms_count + 1, dtype=jnp.int32)
    phase_turns = orders[None, :] * (2 * cycle_index[:, None] + 1) % (2 * cycle_count)
    angles = math.pi * phase_turns.astype(F32) / cycle_count
    orders_real = orders.astype(F32)
    series = jnp.sum(jnp.cos(angles) / (4.0 * orders_real * orders_real - 1.0)[None, :], axis=1)
    return 2.0 / cycle_count * (1.0 - 2.0 * series)


def norm_rows(values, gain):
    average = jnp.mean(values, axis=0, keepdims=True)
    centred = values - average
    variance = jnp.mean(centred * centred, axis=0, keepdims=True)
    return centred * lax.rsqrt(variance + EPSILON) * gain


def analysis_kernel(
    weight_ref, field_ref, gain_ref, cosb_ref, sinb_ref, cosa_ref, sina_ref, out_ref, table_ref, normed_ref, acc_ref
):
    step = pl.program_id(0)

    @pl.when(step == 0)
    def _():
        normed_ref[0:64] = jnp.zeros((64, NLON), BF16)
        normed_ref[256:320] = jnp.zeros((64, NLON), BF16)
        cosb, sinb = cosb_ref[...], sinb_ref[...]
        for part in range(NLON // 128):
            cosa, sina = cosa_ref[:, part : part + 1], sina_ref[:, part : part + 1]
            lanes = slice(128 * part, 128 * part + 128)
            table_ref[0, :, lanes] = (cosa * cosb - sina * sinb).astype(BF16)
            table_ref[1, :, lanes] = (-(sina * cosb + cosa * sinb)).astype(BF16)

    normed_ref[64:256] = norm_rows(field_ref[...].astype(F32), gain_ref[...]).astype(BF16)
    dims = (((1,), (1,)), ((), ()))
    real = lax.dot_general(table_ref[0], normed_ref[64:320], dims, preferred_element_type=F32)
    imag = lax.dot_general(table_ref[1], normed_ref[0:256], dims, preferred_element_type=F32)
    weight = weight_ref[step]
    rows = pl.ds(step, MMAX, stride=ROWS)
    acc_ref[0, rows, :] = real[:, 0:128] * weight
    acc_ref[1, rows, :] = (real[:, 128:256] + imag[:, 0:128]) * weight
    acc_ref[2, rows, :] = imag[:, 128:256] * weight

    @pl.when(step == ROWS - 1)
    def _():
        @pl.loop(0, MMAX * ROWS // 256)
        def _(piece):
            rows = pl.ds(pl.multiple_of(piece * 256, 256), 256)
            for part in range(3):
                out_ref[rows, 128 * part : 128 * part + 128] = acc_ref[part, rows, :].astype(BF16)


def analysis(field, gain, weighting, cosb, sinb, cosa, sina):
    return pl.pallas_call(
        analysis_kernel,
        grid=(ROWS,),
        in_specs=[
            pl.BlockSpec(memory_space=pltpu.SMEM),
            pl.BlockSpec((None, C, NLON), lambda j: (j, 0, 0)),
            whole((C, 1)),
            whole((MMAX, 128)),
            whole((MMAX, 128)),
            whole((MMAX, 8)),
            whole((MMAX, 8)),
        ],
        out_specs=[whole((MMAX * ROWS, K2)), whole((2, MMAX, NLON))],
        out_shape=[
            jax.ShapeDtypeStruct((MMAX * ROWS, K2), BF16),
            jax.ShapeDtypeStruct((2, MMAX, NLON), BF16),
        ],
        scratch_shapes=[pltpu.VMEM((320, NLON), BF16), pltpu.VMEM((3, MMAX * ROWS, 128), F32)],
        compiler_params=params(26),
        cost_estimate=pl.CostEstimate(flops=3_600_000_000, bytes_accessed=9_000_000, transcendentals=0),
        name="analysis",
    )(weighting, field, gain, cosb, sinb, cosa, sina)


def legendre_kernel(orders_ref, cosine_ref, low_ref, start_ref, out_ref, acc_ref, diag_ref):
    step = pl.program_id(0)

    @pl.when(step == 0)
    def _():
        order = [orders_ref[0], orders_ref[1]]
        order_sq = [order[0] * order[0], order[1] * order[1]]
        cosine = cosine_ref[...]
        is_low = low_ref[...] > 0.5
        start = start_ref[...]
        start_level = jnp.floor(start * (1.0 / SCALE_LOG2) + 0.5)
        start_lead = jnp.exp2(start - SCALE_LOG2 * start_level)

        def spread(pair):
            return jnp.where(
                is_low,
                jnp.concatenate([pair[0]] * (LANES // 128), axis=1),
                jnp.concatenate([pair[1]] * (LANES // 128), axis=1),
            )

        order_lanes = spread(order)

        def advance(degree_index, state):
            lead, lag, level = state
            degree = degree_index.astype(F32)
            degree_sq = degree * degree
            degree_norm = jnp.maximum(4.0 * degree_sq - 1.0, 0.0)
            before_sq = (degree - 1.0) * (degree - 1.0)
            before_norm = jnp.maximum(4.0 * before_sq - 1.0, 1.0)
            leading, trailing = [], []
            for one_sq in order_sq:
                lead_coeff = jnp.sqrt(degree_norm / jnp.maximum(degree_sq - one_sq, 1.0))
                leading.append(lead_coeff)
                trailing.append(lead_coeff * jnp.sqrt(jnp.maximum(before_sq - one_sq, 0.0) / before_norm))
            following = spread(leading) * cosine * lead - spread(trailing) * lag
            first = order_lanes == degree
            lag = jnp.where(first, 0.0, lead)
            lead = jnp.where(first, start_lead, following)
            level = jnp.where(first, start_level, level)
            large = jnp.abs(lead) > LIMIT
            lead = jnp.where(large, lead * DOWN, lead)
            lag = jnp.where(large, lag * DOWN, lag)
            level = jnp.where(large, level + 1.0, level)
            value = lead * jnp.where(level > -0.5, 1.0, DOWN)
            value = value * jnp.where(level > -1.5, 1.0, jnp.where(level > -2.5, DOWN, 0.0))
            return (lead, lag, level), value, first

        def position(degree_index):
            odd = lax.rem(degree_index, 2)
            pair = jnp.where(odd == 0, degree_index, LMAX - 1 - degree_index) // 2
            return pl.multiple_of(pair * 16, 16)

        def lower(degree_index, state):
            state, value, _ = advance(degree_index, state)
            rows = pl.ds(position(degree_index) + 8, 8)
            low = jnp.where(is_low, value, 0.0)
            for part in range(LANES // 128):
                acc_ref[part, rows, :] = low[:, 128 * part : 128 * part + 128]
            return state

        def upper(degree_index, state):
            state, value, first = advance(degree_index, state)
            base = position(degree_index)
            low = jnp.where(is_low, value, 0.0)
            high = jnp.where(is_low, 0.0, value)
            added = jnp.where(first, 0.0, high)
            for part in range(LANES // 128):
                lanes = slice(128 * part, 128 * part + 128)
                acc_ref[part, pl.ds(base, 8), :] = low[:, lanes]
                acc_ref[part, pl.ds(base + 8, 8), :] += added[:, lanes]
            diag_ref[...] += jnp.where(first, high, 0.0)
            return state

        diag_ref[...] = jnp.zeros_like(diag_ref)
        zero = jnp.zeros((8, LANES), F32)
        state = lax.fori_loop(0, LMAX // 2, lower, (zero, zero, zero))
        lax.fori_loop(LMAX // 2, LMAX, upper, state)

    for part in range(LANES // 128):
        rows = acc_ref[part, pl.ds(step, T_ROWS, stride=8), :]
        out_ref[0:T_ROWS, 128 * part : 128 * part + 128] = rows.astype(BF16)
    row = lax.broadcasted_iota(jnp.int32, (8, LANES), 0)
    out_ref[T_ROWS:T_PAD] = jnp.where(row == 0, diag_ref[pl.ds(step, 1), :], 0.0).astype(BF16)


def legendre_table(orders, cosine, low, start):
    return pl.pallas_call(
        legendre_kernel,
        grid=(PAIRS,),
        in_specs=[whole((2, 8, 128)), whole((8, LANES)), whole((8, LANES)), whole((8, LANES))],
        out_specs=pl.BlockSpec((None, T_PAD, LANES), lambda i: (i, 0, 0)),
        out_shape=jax.ShapeDtypeStruct((PAIRS, T_PAD, LANES), BF16),
        scratch_shapes=[pltpu.VMEM((LANES // 128, T_ROWS * 8, 128), F32), pltpu.VMEM((8, LANES), F32)],
        compiler_params=params(22),
        cost_estimate=pl.CostEstimate(flops=10_000_000_000, bytes_accessed=4_000_000, transcendentals=0),
        name="legendre_table",
    )(orders, cosine, low, start)


def forward_kernel(table_ref, spectral_ref, out_ref, diag_ref, acc_ref):
    step = pl.program_id(0)
    values = spectral_ref[...].reshape(LANES, K2)
    result = jnp.dot(table_ref[...], values, preferred_element_type=F32)
    for part in range(3):
        acc_ref[part, pl.ds(step, T_ROWS, stride=PAIRS), :] = result[0:T_ROWS, 128 * part : 128 * part + 128]
    row = lax.broadcasted_iota(jnp.int32, (8, K2), 0)

    @pl.when(step == 0)
    def _():
        diag_ref[...] = jnp.zeros_like(diag_ref)

    diag_ref[...] = jnp.where(row == step, result[T_ROWS : T_ROWS + 1], diag_ref[...])

    @pl.when(step == PAIRS - 1)
    def _():
        @pl.loop(0, SP * BLOCK_L // 256)
        def _(piece):
            rows = pl.ds(pl.multiple_of(piece * 256, 256), 256)
            for part in range(3):
                out_ref[rows, 128 * part : 128 * part + 128] = acc_ref[part, rows, :].astype(BF16)


def forward(table, spectral):
    return pl.pallas_call(
        forward_kernel,
        grid=(PAIRS,),
        in_specs=[
            pl.BlockSpec((None, T_PAD, LANES), lambda i: (i, 0, 0)),
            pl.BlockSpec((SP, None, 2 * ROWS, K2), lambda i: (0, i, 0, 0)),
        ],
        out_specs=[whole((SP * BLOCK_L, K2)), whole((8, K2))],
        out_shape=[jax.ShapeDtypeStruct((SP * BLOCK_L, K2), BF16), jax.ShapeDtypeStruct((8, K2), F32)],
        scratch_shapes=[pltpu.VMEM((3, SP * BLOCK_L, 128), F32)],
        compiler_params=params(16),
        cost_estimate=pl.CostEstimate(flops=1_400_000_000, bytes_accessed=9_000_000, transcendentals=0),
        name="forward",
    )(table, spectral)


def mixing_kernel(rank_ref, coeffs_ref, own_ref, other_ref, diag_ref, out_ref, diag_out_ref):
    step = pl.program_id(0)
    rank = rank_ref[0]
    own_is_low = rank < SP // 2
    values = coeffs_ref[...].reshape(SP * 24, K2)
    index = lax.broadcasted_iota(jnp.int32, (SP * 24, 1), 0)
    owner = index // 24
    within = index - owner * 24
    local = within // 12
    within = within - local * 12
    second = within // 6
    order = pair_low(owner * PAIRS + within - second * 6)
    low_degree = pair_low(rank * PAIRS + 2 * step + local)
    uses_low = jnp.logical_and(second == 1, order <= low_degree)
    uses_own = uses_low == own_is_low
    result = []
    for pair in range(2):
        own = jnp.dot(values, own_ref[pair], preferred_element_type=F32)
        other = jnp.dot(values, other_ref[pair], preferred_element_type=F32)
        result.append(jnp.where(uses_own, own, other))
    mixed = jnp.where(local == 0, result[0], result[1]).astype(BF16)
    out_ref[...] = mixed.reshape(SP, 24, K2)

    @pl.when(step == 0)
    def _():
        diag_out_ref[...] = jnp.zeros_like(diag_out_ref)

    diag = diag_ref[...].astype(BF16)
    row = lax.broadcasted_iota(jnp.int32, (8, K2), 0)
    for pair in range(2):
        own = jnp.dot(diag, own_ref[pair], preferred_element_type=F32)
        other = jnp.dot(diag, other_ref[pair], preferred_element_type=F32)
        chosen = jnp.where(own_is_low, other, own)
        diag_out_ref[...] = jnp.where(row == 2 * step + pair, chosen, diag_out_ref[...])


def mixing(rank, coeffs, own, other, diag):
    block = pl.BlockSpec((SP, 24, K2), lambda g: (0, g, 0))
    weight = pl.BlockSpec((2, K2, K2), lambda g: (g, 0, 0))
    return pl.pallas_call(
        mixing_kernel,
        grid=(PAIRS // 2,),
        in_specs=[pl.BlockSpec(memory_space=pltpu.SMEM), block, weight, weight, whole((8, K2))],
        out_specs=[block, whole((8, K2))],
        out_shape=[jax.ShapeDtypeStruct((SP, BLOCK_L, K2), BF16), jax.ShapeDtypeStruct((8, K2), F32)],
        compiler_params=params(20),
        cost_estimate=pl.CostEstimate(flops=2_700_000_000, bytes_accessed=7_000_000, transcendentals=0),
        name="mixing",
    )(rank, coeffs, own, other, diag)


def inverse_kernel(table_ref, mixed_ref, diag_ref, out_ref, acc_ref):
    step = pl.program_id(0)

    @pl.when(step == 0)
    def _():
        @pl.loop(0, SP * BLOCK_L // 256)
        def _(piece):
            rows = pl.ds(pl.multiple_of(piece * 256, 256), 256)
            for part in range(3):
                acc_ref[part, rows, :] = mixed_ref[rows, 128 * part : 128 * part + 128].astype(F32)

    rows = pl.ds(step, T_ROWS, stride=PAIRS)
    values = jnp.concatenate([acc_ref[part, rows, :] for part in range(3)], axis=1).astype(BF16)
    row = lax.broadcasted_iota(jnp.int32, (8, K2), 0)
    diag = jnp.where(row == 0, diag_ref[pl.ds(step, 1), :], 0.0).astype(BF16)
    dims = (((0,), (0,)), ((), ()))
    result = lax.dot_general(table_ref[0:T_ROWS], values, dims, preferred_element_type=F32)
    result += lax.dot_general(table_ref[T_ROWS:T_PAD], diag, dims, preferred_element_type=F32)
    out_ref[...] = result.astype(BF16).reshape(SP, 2 * ROWS, K2)


def inverse(table, mixed, diag):
    return pl.pallas_call(
        inverse_kernel,
        grid=(PAIRS,),
        in_specs=[
            pl.BlockSpec((None, T_PAD, LANES), lambda i: (i, 0, 0)),
            whole((SP * BLOCK_L, K2)),
            whole((8, K2)),
        ],
        out_specs=pl.BlockSpec((SP, None, 2 * ROWS, K2), lambda i: (0, i, 0, 0)),
        out_shape=jax.ShapeDtypeStruct((SP, PAIRS, 2 * ROWS, K2), BF16),
        scratch_shapes=[pltpu.VMEM((3, SP * BLOCK_L, 128), F32)],
        compiler_params=params(18),
        cost_estimate=pl.CostEstimate(flops=1_400_000_000, bytes_accessed=9_000_000, transcendentals=0),
        name="inverse",
    )(table, mixed, diag)


def synthesis_kernel(
    grid_ref, field_ref, table_ref, gain_ref, up_ref, bias_ref, down_ref, out_ref, acc_ref
):
    step = pl.program_id(0)

    @pl.when(step == 0)
    def _():
        @pl.loop(0, MMAX * ROWS // 256)
        def _(piece):
            rows = pl.ds(pl.multiple_of(piece * 256, 256), 256)
            for part in range(3):
                acc_ref[part, rows, :] = grid_ref[rows, 128 * part : 128 * part + 128].astype(F32)

    rows = pl.ds(step, MMAX, stride=ROWS)
    values = jnp.concatenate([acc_ref[part, rows, :] for part in range(3)], axis=1)
    row = lax.broadcasted_iota(jnp.int32, (MMAX, K2), 0)
    values = jnp.where(row == 0, values, 2.0 * values)
    turned = values.T.astype(BF16)
    residual = field_ref[...].astype(F32)
    residual += jnp.dot(turned[0:C], table_ref[0], preferred_element_type=F32)
    residual += jnp.dot(turned[C:K2], table_ref[1], preferred_element_type=F32)
    hidden_in = norm_rows(residual, gain_ref[...]).astype(BF16)
    hidden = jnp.dot(up_ref[...], hidden_in, preferred_element_type=F32) + bias_ref[...]
    hidden = hidden * (1.0 + lax.erf(hidden * math.sqrt(0.5))) * 0.5
    branch = jnp.dot(down_ref[...], hidden.astype(BF16), preferred_element_type=F32)
    out_ref[...] = (residual + branch).astype(BF16)


def synthesis(on_grid, field, table, gain, up, bias, down):
    cycle = pl.BlockSpec((None, C, NLON), lambda j: (j, 0, 0))
    return pl.pallas_call(
        synthesis_kernel,
        grid=(ROWS,),
        in_specs=[
            whole((MMAX * ROWS, K2)),
            cycle,
            whole((2, MMAX, NLON)),
            whole((C, 1)),
            whole((HID, C)),
            whole((HID, 1)),
            whole((C, HID)),
        ],
        out_specs=cycle,
        out_shape=jax.ShapeDtypeStruct((ROWS, C, NLON), BF16),
        scratch_shapes=[pltpu.VMEM((3, MMAX * ROWS, 128), F32)],
        compiler_params=params(32),
        cost_estimate=pl.CostEstimate(flops=8_000_000_000, bytes_accessed=12_000_000, transcendentals=0),
        name="synthesis",
    )(on_grid, field, table, gain, up, bias, down)


def mixing_matrix(weight):
    real_weight = weight[:, :, :C]
    imag_weight = weight[:, :, C:]
    bottom_half = jnp.concatenate([-imag_weight, real_weight], axis=2)
    return jnp.concatenate([weight, bottom_half], axis=1)


def to_next(value):
    count = lax.axis_size("section")
    return lax.ppermute(value, "section", [(i, (i + 1) % count) for i in range(count)])


def to_mirrored(value):
    count = lax.axis_size("sp")
    return lax.ppermute(value, "sp", [(d, count - 1 - d) for d in range(count)])


def exchange(value):
    return lax.all_to_all(value, "sp", split_axis=0, concat_axis=0)


def legendre_inputs(rank):
    pair = rank * PAIRS + jnp.minimum(jnp.arange(8, dtype=jnp.int32), PAIRS - 1)
    orders = jnp.stack([pair_low(pair), pair_high(pair)]).astype(F32)
    lane = jnp.arange(LANES, dtype=jnp.int32)
    low = (lane // ROWS) % 2 == 0
    cycle = lane // (2 * ROWS) * ROWS + lane % ROWS
    colatitude = math.pi * (cycle.astype(F32) + 0.5) / NLAT
    steps_all = jnp.arange(1, LMAX + 1, dtype=F32)
    factors = jnp.log((2.0 * steps_all - 1.0) / (2.0 * steps_all))
    below = (steps_all <= orders[:, :, None]).astype(F32)
    partial_log = jnp.sum(below * factors, axis=2)
    start = 0.5 * jnp.log((2.0 * orders + 1.0) / (4.0 * math.pi)) + 0.5 * partial_log
    order_lanes = jnp.where(low, orders[0][:, None], orders[1][:, None])
    start = jnp.where(low, start[0][:, None], start[1][:, None])
    start = (start + order_lanes * jnp.log(jnp.sin(colatitude))) * (1.0 / math.log(2.0))
    return (
        jnp.broadcast_to(orders[:, :, None], (2, 8, 128)),
        jnp.broadcast_to(jnp.cos(colatitude), (8, LANES)),
        jnp.broadcast_to(low.astype(F32), (8, LANES)),
        start,
    )


def fourier_inputs():
    pair = jnp.arange(MMAX // 2, dtype=jnp.int32)
    orders = jnp.stack([pair_low(pair), pair_high(pair)], axis=1).reshape(MMAX, 1)
    fine = (2.0 * math.pi / NLON) * (orders * jnp.arange(128, dtype=jnp.int32) % NLON).astype(F32)
    coarse = (2.0 * math.pi / 6) * (orders * jnp.arange(8, dtype=jnp.int32) % 6).astype(F32)
    return (jnp.cos(fine), jnp.sin(fine), jnp.cos(coarse), jnp.sin(coarse))


def block(field_in, spectral_gain, spectral_weight, mixer_gain, up_weight, up_bias, down_weight):
    field = field_in[0]
    rank = lax.axis_index("sp")
    weighting = quad_weights(rank * ROWS + jnp.arange(ROWS, dtype=jnp.int32), NLAT) * (2.0 * math.pi / NLON)
    spectral, table = analysis(
        field, spectral_gain.reshape(C, 1).astype(F32), weighting, *fourier_inputs()
    )
    rank_after, weight, _ = lax.optimization_barrier((rank, spectral_weight[0], spectral))
    by_order = exchange(spectral.reshape(SP, BLOCK_M, K2))
    weight = to_next(weight)
    own_weight, other_weight = weight[0::2], weight[1::2][::-1]
    legendre = legendre_table(*legendre_inputs(rank_after))

    by_order, other_weight = lax.optimization_barrier((by_order, other_weight))
    other_weight = to_mirrored(other_weight)
    coeffs, diag = forward(legendre, by_order.reshape(SP, PAIRS, 2 * ROWS, K2))
    coeffs = to_next(coeffs)
    diag = to_next(diag)
    by_degree = exchange(coeffs.reshape(SP, BLOCK_L, K2))
    own_matrix, other_matrix = mixing_matrix(own_weight), mixing_matrix(other_weight)
    mixed, diag = mixing(rank.reshape(1), by_degree, own_matrix, other_matrix, diag)
    back = exchange(mixed)
    grid_part = inverse(legendre, back.reshape(SP * BLOCK_L, K2), diag)
    on_grid = exchange(grid_part.reshape(SP, BLOCK_M, K2))
    next_field = to_next(field)
    gain_next, bias_next = to_next(mixer_gain), to_next(up_bias)
    up_next, down_next = to_next(up_weight), to_next(down_weight)
    result = synthesis(
        on_grid.reshape(MMAX * ROWS, K2),
        next_field,
        table,
        gain_next.reshape(C, 1).astype(F32),
        up_next[0].T,
        bias_next.reshape(HID, 1).astype(F32),
        down_next[0],
    )
    return result[None]


def solution(mesh):
    in_specs = (
        P("section", "sp", None, None),
        P("section", None),
        P("section", "sp", None, None),
        P("section", None),
        P("section", None, None),
        P("section", None),
        P("section", None, None),
    )
    out_specs = P("section", "sp", None, None)
    return jax.shard_map(block, mesh=mesh, in_specs=in_specs, out_specs=out_specs, check_vma=False)
```

```python
import functools
import math

import jax
import jax.numpy as jnp
from jax import lax
from jax.experimental import pallas as pl
from jax.experimental.pallas import tpu as pltpu
from jax.sharding import PartitionSpec as P


C = 192
HID = 384
NLAT = 384
NLON = 768
LMAX = 384
MMAX = 384
SP = 32
ROWS = NLAT // SP
PAIRS = LMAX // SP // 2
K2 = 2 * C
BLOCK_M = 2 * PAIRS * ROWS
BLOCK_L = 2 * PAIRS * PAIRS
EARLY = 2
T_ROWS = LMAX
T_PAD = T_ROWS + 8
LANES = 2 * NLAT

EPSILON = 1e-05
SCALE_LOG2 = 64.0
DOWN = 2.0**-64
LIMIT = 2.0**32

F32 = jnp.float32
BF16 = jnp.bfloat16


def pair_low(pair):
    degree = pair + pair // PAIRS * PAIRS
    return jnp.minimum(degree, LMAX - 1 - degree)


def pair_high(pair):
    degree = pair + pair // PAIRS * PAIRS
    return jnp.maximum(degree, LMAX - 1 - degree)


def params(mebibytes):
    return pltpu.CompilerParams(vmem_limit_bytes=mebibytes * 1024 * 1024)


def in_hbm(value):
    return pltpu.with_memory_space_constraint(value, pltpu.HBM)


IN_VMEM = pl.BlockSpec(memory_space=pltpu.VMEM)


def whole(shape):
    return pl.BlockSpec(shape, lambda *_: (0,) * len(shape))


def norm_rows(values, gain):
    average = jnp.mean(values, axis=0, keepdims=True)
    centred = values - average
    variance = jnp.mean(centred * centred, axis=0, keepdims=True)
    return centred * lax.rsqrt(variance + EPSILON) * gain


def remainder(values, by):
    return values - by * jnp.floor(values * (1.0 / by))


def fill_fourier_table(table_ref, scale):
    row = lax.broadcasted_iota(jnp.int32, (MMAX, 128), 0)
    pair = lax.shift_right_logical(row, 1)
    order = jnp.where(lax.bitwise_and(row, 1) == 0, pair_low(pair), pair_high(pair)).astype(F32)
    lane = lax.broadcasted_iota(jnp.int32, (MMAX, 128), 1).astype(F32)
    angle = remainder(order * lane, float(NLON)) * (2.0 * math.pi / NLON)
    factor = jnp.where(order == 0.0, 1.0, scale)
    cosine, sine = jnp.cos(angle) * factor, jnp.sin(angle) * factor
    sixth = jnp.floor(remainder(order, 6.0) + 0.5)
    half = jnp.where((sixth == 1.0) | (sixth == 5.0), 0.5, -0.5)
    turn_cos = jnp.where(sixth == 0.0, 1.0, jnp.where(sixth == 3.0, -1.0, half))
    root = math.sqrt(0.75)
    turn_sin = jnp.where((sixth == 0.0) | (sixth == 3.0), 0.0, jnp.where(sixth < 3.0, root, -root))
    for part in range(NLON // 128):
        lanes = slice(128 * part, 128 * part + 128)
        table_ref[0:MMAX, lanes] = cosine.astype(BF16)
        table_ref[MMAX : 2 * MMAX, lanes] = (-sine).astype(BF16)
        cosine, sine = cosine * turn_cos - sine * turn_sin, sine * turn_cos + cosine * turn_sin


def cycle_weights(rank):
    cycle = lax.broadcasted_iota(jnp.int32, (16, 256), 0) + rank * ROWS
    term = (lax.broadcasted_iota(jnp.int32, (16, 256), 1) + 1).astype(F32)
    turns = remainder(term * (2 * cycle + 1).astype(F32), 2.0 * NLAT)
    parts = jnp.cos(turns * (math.pi / NLAT)) / (4.0 * term * term - 1.0)
    series = jnp.sum(jnp.where(term <= NLAT // 2, parts, 0.0), axis=1, keepdims=True)
    return 2.0 / NLAT * (1.0 - 2.0 * series) * (2.0 * math.pi / NLON)


def analysis_kernel(
    rank_ref, field_ref, gain_ref, out_ref, table_ref, weight_ref, column_ref, normed_ref, acc_ref
):
    step = pl.program_id(0)

    @pl.when(step == 0)
    def _():
        for half in range(2):
            normed_ref[half, 0:64] = jnp.zeros((64, NLON), BF16)
            normed_ref[half, 256:320] = jnp.zeros((64, NLON), BF16)
        fill_fourier_table(table_ref, 1.0)
        weight_ref[...] = jnp.broadcast_to(cycle_weights(rank_ref[0]), (16, 128))
        same = lax.broadcasted_iota(jnp.int32, (C, C), 0) == lax.broadcasted_iota(jnp.int32, (C, C), 1)
        column = jnp.sum(jnp.where(same, gain_ref[...].astype(F32), 0.0), axis=1, keepdims=True)
        column_ref[...] = jnp.broadcast_to(column, (C, 128))

    @pl.when(step < ROWS // 2)
    def _():
        dims = (((1,), (1,)), ((), ()))
        gain = jnp.concatenate([column_ref[...]] * (NLON // 128), axis=1)
        for half in range(2):
            normed_ref[half, 64:256] = norm_rows(field_ref[half].astype(F32), gain).astype(BF16)
        for half in range(2):
            cycle = 2 * step + half
            weight = weight_ref[pl.ds(cycle, 1), :]
            rows = pl.ds(cycle, MMAX, stride=ROWS)
            real = lax.dot_general(
                table_ref[0:MMAX], normed_ref[half, 64:320], dims, preferred_element_type=F32
            )
            imag = lax.dot_general(
                table_ref[MMAX : 2 * MMAX], normed_ref[half, 0:256], dims, preferred_element_type=F32
            )
            acc_ref[0, rows, :] = real[:, 0:128] * weight
            acc_ref[1, rows, :] = (real[:, 128:256] + imag[:, 0:128]) * weight
            acc_ref[2, rows, :] = imag[:, 128:256] * weight

    @pl.when(step >= ROWS // 2)
    def _():
        base = (step - ROWS // 2) * (MMAX * ROWS // 6)

        @pl.loop(0, MMAX * ROWS // 6 // 128)
        def _(piece):
            into = pl.ds(pl.multiple_of(piece * 128, 128), 128)
            rows = pl.ds(pl.multiple_of(base + piece * 128, 128), 128)
            for part in range(3):
                out_ref[into, 128 * part : 128 * part + 128] = acc_ref[part, rows, :].astype(BF16)


def analysis(rank, field, gain):
    steps = ROWS // 2
    return pl.pallas_call(
        analysis_kernel,
        grid=(steps + 6,),
        in_specs=[
            pl.BlockSpec(memory_space=pltpu.SMEM),
            pl.BlockSpec((2, C, NLON), lambda j: (jnp.minimum(j, steps - 1), 0, 0)),
            whole((1, C)),
        ],
        out_specs=pl.BlockSpec((MMAX * ROWS // 6, K2), lambda j: (jnp.maximum(j - steps, 0), 0)),
        out_shape=pltpu.HBM((MMAX * ROWS, K2), BF16),
        scratch_shapes=[
            pltpu.VMEM((2 * MMAX, NLON), BF16),
            pltpu.VMEM((16, 128), F32),
            pltpu.VMEM((C, 128), F32),
            pltpu.VMEM((2, 320, NLON), BF16),
            pltpu.VMEM((3, MMAX * ROWS, 128), F32),
        ],
        compiler_params=params(28),
        cost_estimate=pl.CostEstimate(flops=3_600_000_000, bytes_accessed=9_000_000, transcendentals=0),
        name="analysis",
    )(rank, in_hbm(field), gain)


def legendre_kernel(orders_ref, cosine_ref, low_ref, start_ref, out_ref, fourier_ref, acc_ref, diag_ref):
    step = pl.program_id(0)

    @pl.when(step == 0)
    def _():
        fill_fourier_table(fourier_ref, 2.0)
        order = [orders_ref[0], orders_ref[1]]
        order_sq = [order[0] * order[0], order[1] * order[1]]
        cosine = cosine_ref[...]
        is_low = low_ref[...] > 0.5
        start = start_ref[...]
        start_level = jnp.floor(start * (1.0 / SCALE_LOG2) + 0.5)
        start_lead = jnp.exp2(start - SCALE_LOG2 * start_level)

        def spread(pair):
            return jnp.where(
                is_low,
                jnp.concatenate([pair[0]] * (LANES // 128), axis=1),
                jnp.concatenate([pair[1]] * (LANES // 128), axis=1),
            )

        order_lanes = spread(order)

        def advance(degree_index, state):
            lead, lag, level = state
            degree = degree_index.astype(F32)
            degree_sq = degree * degree
            degree_norm = jnp.maximum(4.0 * degree_sq - 1.0, 0.0)
            before_sq = (degree - 1.0) * (degree - 1.0)
            before_norm = jnp.maximum(4.0 * before_sq - 1.0, 1.0)
            leading, trailing = [], []
            for one_sq in order_sq:
                lead_coeff = jnp.sqrt(degree_norm / jnp.maximum(degree_sq - one_sq, 1.0))
                leading.append(lead_coeff)
                trailing.append(lead_coeff * jnp.sqrt(jnp.maximum(before_sq - one_sq, 0.0) / before_norm))
            following = spread(leading) * cosine * lead - spread(trailing) * lag
            first = order_lanes == degree
            lag = jnp.where(first, 0.0, lead)
            lead = jnp.where(first, start_lead, following)
            level = jnp.where(first, start_level, level)
            large = jnp.abs(lead) > LIMIT
            lead = jnp.where(large, lead * DOWN, lead)
            lag = jnp.where(large, lag * DOWN, lag)
            level = jnp.where(large, level + 1.0, level)
            value = lead * jnp.where(level > -0.5, 1.0, DOWN)
            value = value * jnp.where(level > -1.5, 1.0, jnp.where(level > -2.5, DOWN, 0.0))
            return (lead, lag, level), value, first

        def position(degree_index):
            mirrored = lax.rem(degree_index, 2 * PAIRS) >= PAIRS
            degree = jnp.where(mirrored, LMAX - 1 - degree_index, degree_index)
            pair = degree - degree // (2 * PAIRS) * PAIRS
            return pl.multiple_of(pair * 16, 16)

        def lower(degree_index, state):
            state, value, _ = advance(degree_index, state)
            rows = pl.ds(position(degree_index) + 8, 8)
            low = jnp.where(is_low, value, 0.0)
            for part in range(LANES // 128):
                acc_ref[part, rows, :] = low[:, 128 * part : 128 * part + 128]
            return state

        def upper(degree_index, state):
            state, value, first = advance(degree_index, state)
            base = position(degree_index)
            low = jnp.where(is_low, value, 0.0)
            high = jnp.where(is_low, 0.0, value)
            added = jnp.where(first, 0.0, high)
            for part in range(LANES // 128):
                lanes = slice(128 * part, 128 * part + 128)
                acc_ref[part, pl.ds(base, 8), :] = low[:, lanes]
                acc_ref[part, pl.ds(base + 8, 8), :] += added[:, lanes]
            diag_ref[...] += jnp.where(first, high, 0.0)
            return state

        diag_ref[...] = jnp.zeros_like(diag_ref)
        zero = jnp.zeros((8, LANES), F32)
        state = lax.fori_loop(0, LMAX // 2, lower, (zero, zero, zero))
        lax.fori_loop(LMAX // 2, LMAX, upper, state)

    for part in range(LANES // 128):
        rows = acc_ref[part, pl.ds(step, T_ROWS, stride=8), :]
        out_ref[0:T_ROWS, 128 * part : 128 * part + 128] = rows.astype(BF16)
    row = lax.broadcasted_iota(jnp.int32, (8, LANES), 0)
    out_ref[T_ROWS:T_PAD] = jnp.where(row == 0, diag_ref[pl.ds(step, 1), :], 0.0).astype(BF16)


def legendre_table(orders, cosine, low, start):
    return pl.pallas_call(
        legendre_kernel,
        grid=(PAIRS,),
        in_specs=[whole((2, 8, 128)), whole((8, LANES)), whole((8, LANES)), whole((8, LANES))],
        out_specs=[
            pl.BlockSpec((None, T_PAD, LANES), lambda i: (i, 0, 0)),
            whole((2 * MMAX, NLON)),
        ],
        out_shape=[pltpu.HBM((PAIRS, T_PAD, LANES), BF16), pltpu.HBM((2 * MMAX, NLON), BF16)],
        scratch_shapes=[pltpu.VMEM((LANES // 128, T_ROWS * 8, 128), F32), pltpu.VMEM((8, LANES), F32)],
        compiler_params=params(22),
        cost_estimate=pl.CostEstimate(flops=10_000_000_000, bytes_accessed=4_000_000, transcendentals=0),
        name="legendre_table",
    )(orders, cosine, low, start)


def forward_kernel(first, count, table_ref, spectral_ref, out_ref, diag_ref, acc_ref):
    step = pl.program_id(0)
    values = spectral_ref[:, first + step].reshape(LANES, K2)
    result = jnp.dot(table_ref[...], values, preferred_element_type=F32)
    for part in range(3):
        acc_ref[part, pl.ds(step, T_ROWS, stride=count), :] = result[0:T_ROWS, 128 * part : 128 * part + 128]
    row = lax.broadcasted_iota(jnp.int32, (8, K2), 0)

    @pl.when(step == 0)
    def _():
        diag_ref[...] = jnp.zeros_like(diag_ref)

    diag_ref[...] = jnp.where(row == first + step, result[T_ROWS : T_ROWS + 1], diag_ref[...])

    @pl.when(step == count - 1)
    def _():
        @pl.loop(0, T_ROWS * count // 256)
        def _(piece):
            rows = pl.ds(pl.multiple_of(piece * 256, 256), 256)
            for part in range(3):
                out_ref[rows, 128 * part : 128 * part + 128] = acc_ref[part, rows, :].astype(BF16)


def forward(table, spectral, first, count):
    return pl.pallas_call(
        functools.partial(forward_kernel, first, count),
        grid=(count,),
        in_specs=[pl.BlockSpec((None, T_PAD, LANES), lambda i: (first + i, 0, 0)), IN_VMEM],
        out_specs=[whole((T_ROWS * count, K2)), whole((8, K2))],
        out_shape=[pltpu.HBM((T_ROWS * count, K2), BF16), jax.ShapeDtypeStruct((8, K2), F32)],
        scratch_shapes=[pltpu.VMEM((3, T_ROWS * count, 128), F32)],
        compiler_params=params(14),
        cost_estimate=pl.CostEstimate(
            flops=230_000_000 * count, bytes_accessed=1_500_000 * count, transcendentals=0
        ),
        name="forward",
    )(in_hbm(table), spectral)


def mixing_choice(rank, first, count):
    block = 4 * count
    step = jnp.arange(PAIRS // 2, dtype=jnp.int32)[:, None]
    index = jnp.arange(SP * block, dtype=jnp.int32)[None, :]
    within = index % block
    local = within // (2 * count)
    second = within // count % 2
    order = pair_low(index // block * PAIRS + first + within % count)
    low_degree = pair_low(rank * PAIRS + 2 * step + local)
    uses_low = jnp.logical_and(second == 1, order <= low_degree)
    uses_own = uses_low == (rank < SP // 2)
    choice = (2 * local + uses_own.astype(jnp.int32)).astype(F32)
    return jnp.broadcast_to(choice[:, :, None], (PAIRS // 2, SP * block, 128))


def mixing_kernel(count, rank_ref, coeffs_ref, choice_ref, own_ref, other_ref, diag_ref, *refs):
    out_ref, diag_out_ref = refs[-2:]
    step = pl.program_id(0)
    block = 4 * count
    values = coeffs_ref[:, pl.ds(pl.multiple_of(block * step, 8), block), :].reshape(SP * block, K2)
    choice = jnp.concatenate([choice_ref[...]] * (K2 // 128), axis=1)
    result = []
    for pair in range(2):
        own = jnp.dot(values, own_ref[2 * step + pair], preferred_element_type=F32)
        other = jnp.dot(values, other_ref[PAIRS - 1 - 2 * step - pair], preferred_element_type=F32)
        result.append(jnp.where(choice == 2.0 * pair, other, own))
    mixed = jnp.where(choice < 1.5, result[0], result[1]).astype(BF16)
    out_ref[...] = mixed.reshape(SP, block, K2)

    if len(refs) == 2:
        own_is_low = rank_ref[0] < SP // 2

        @pl.when(step == 0)
        def _():
            diag_out_ref[...] = jnp.zeros_like(diag_out_ref)

        diag = diag_ref[...].astype(BF16)
        row = lax.broadcasted_iota(jnp.int32, (8, K2), 0)
        for pair in range(2):
            own = jnp.dot(diag, own_ref[2 * step + pair], preferred_element_type=F32)
            other = jnp.dot(diag, other_ref[PAIRS - 1 - 2 * step - pair], preferred_element_type=F32)
            chosen = jnp.where(own_is_low, other, own)
            diag_out_ref[...] = jnp.where(row == 2 * step + pair, chosen, diag_out_ref[...])
    else:
        diag_out_ref[...] = diag_ref[...]


def mixing(rank, coeffs, choice, own, other, diag, count, offset, filled=None):
    block = 4 * count
    extra = [] if filled is None else [filled]
    return pl.pallas_call(
        functools.partial(mixing_kernel, count),
        grid=(PAIRS // 2,),
        in_specs=[
            pl.BlockSpec(memory_space=pltpu.SMEM),
            IN_VMEM,
            pl.BlockSpec((None, SP * block, 128), lambda g: (g, 0, 0)),
            IN_VMEM,
            IN_VMEM,
            whole((8, K2)),
        ]
        + [pl.BlockSpec(memory_space=pl.ANY) for _ in extra],
        out_specs=[pl.BlockSpec((SP, block, K2), lambda g: (0, offset // block + g, 0)), whole((8, K2))],
        out_shape=[pltpu.HBM((SP, BLOCK_L, K2), BF16), jax.ShapeDtypeStruct((8, K2), F32)],
        input_output_aliases={6: 0} if extra else {},
        compiler_params=params(14),
        cost_estimate=pl.CostEstimate(
            flops=450_000_000 * count, bytes_accessed=1_200_000 * count, transcendentals=0
        ),
        name="mixing",
    )(rank, coeffs, in_hbm(choice), own, other, diag, *extra)


def inverse_kernel(table_ref, mixed_ref, diag_ref, out_ref, early_ref, late_ref, values_ref):
    step = pl.program_id(0)
    split = BLOCK_L // PAIRS * (PAIRS - EARLY)
    rest = BLOCK_L - split

    @pl.when(step == 0)
    def _():
        @pl.loop(0, SP)
        def _(owner):
            early = pl.ds(pl.multiple_of(owner * split, 8), split)
            late = pl.ds(pl.multiple_of(owner * rest, 8), rest)
            for part in range(3):
                lanes = slice(128 * part, 128 * part + 128)
                early_ref[part, early, :] = mixed_ref[owner, 0:split, lanes].astype(F32)
                late_ref[part, late, :] = mixed_ref[owner, split:BLOCK_L, lanes].astype(F32)

    @pl.when(step < EARLY)
    def _():
        rows = pl.ds(step, T_ROWS, stride=EARLY)
        for part in range(3):
            values_ref[:, 128 * part : 128 * part + 128] = late_ref[part, rows, :].astype(BF16)

    @pl.when(step >= EARLY)
    def _():
        rows = pl.ds(step - EARLY, T_ROWS, stride=PAIRS - EARLY)
        for part in range(3):
            values_ref[:, 128 * part : 128 * part + 128] = early_ref[part, rows, :].astype(BF16)

    row = lax.broadcasted_iota(jnp.int32, (8, K2), 0)
    diag = jnp.where(row == 0, diag_ref[pl.ds(step, 1), :], 0.0).astype(BF16)
    dims = (((0,), (0,)), ((), ()))
    result = lax.dot_general(table_ref[step, 0:T_ROWS], values_ref[...], dims, preferred_element_type=F32)
    result += lax.dot_general(table_ref[step, T_ROWS:T_PAD], diag, dims, preferred_element_type=F32)
    out_ref[...] = result.astype(BF16).reshape(SP, 2 * ROWS, K2)


def inverse(table, mixed, diag):
    return pl.pallas_call(
        inverse_kernel,
        grid=(PAIRS,),
        in_specs=[IN_VMEM, IN_VMEM, whole((8, K2))],
        out_specs=pl.BlockSpec((SP, None, 2 * ROWS, K2), lambda i: (0, i, 0, 0)),
        out_shape=pltpu.HBM((SP, PAIRS, 2 * ROWS, K2), BF16),
        scratch_shapes=[
            pltpu.VMEM((3, T_ROWS * (PAIRS - EARLY), 128), F32),
            pltpu.VMEM((3, T_ROWS * EARLY, 128), F32),
            pltpu.VMEM((T_ROWS, K2), BF16),
        ],
        compiler_params=params(16),
        cost_estimate=pl.CostEstimate(flops=1_400_000_000, bytes_accessed=9_000_000, transcendentals=0),
        name="inverse",
    )(table, mixed, diag)


def synthesis_kernel(
    grid_ref, field_ref, table_ref, gain_ref, up_ref, bias_ref, down_ref, out_ref, acc_ref
):
    step = pl.program_id(0)

    @pl.when(step == 0)
    def _():
        @pl.loop(0, MMAX * ROWS // 256)
        def _(piece):
            rows = pl.ds(pl.multiple_of(piece * 256, 256), 256)
            for part in range(3):
                acc_ref[part, rows, :] = grid_ref[rows, 128 * part : 128 * part + 128].astype(F32)

    residuals = []
    for half in range(2):
        rows = pl.ds(2 * step + half, MMAX, stride=ROWS)
        values = jnp.concatenate([acc_ref[part, rows, :] for part in range(3)], axis=1)
        turned = values.T.astype(BF16)
        residual = field_ref[half].astype(F32)
        residual += jnp.dot(turned[0:C], table_ref[0:MMAX], preferred_element_type=F32)
        residual += jnp.dot(turned[C:K2], table_ref[MMAX : 2 * MMAX], preferred_element_type=F32)
        residuals.append(residual)
    for half in range(2):
        hidden_in = norm_rows(residuals[half], gain_ref[...]).astype(BF16)
        hidden = jnp.dot(up_ref[...], hidden_in, preferred_element_type=F32) + bias_ref[...]
        hidden = hidden * (1.0 + lax.erf(hidden * math.sqrt(0.5))) * 0.5
        branch = jnp.dot(down_ref[...], hidden.astype(BF16), preferred_element_type=F32)
        out_ref[half] = (residuals[half] + branch).astype(BF16)


def synthesis(on_grid, field, table, gain, up, bias, down):
    cycle = pl.BlockSpec((2, C, NLON), lambda j: (j, 0, 0))
    return pl.pallas_call(
        synthesis_kernel,
        grid=(ROWS // 2,),
        in_specs=[
            IN_VMEM,
            cycle,
            whole((2 * MMAX, NLON)),
            whole((C, 1)),
            whole((HID, C)),
            whole((HID, 1)),
            whole((C, HID)),
        ],
        out_specs=cycle,
        out_shape=jax.ShapeDtypeStruct((ROWS, C, NLON), BF16),
        scratch_shapes=[pltpu.VMEM((3, MMAX * ROWS, 128), F32)],
        compiler_params=params(32),
        cost_estimate=pl.CostEstimate(flops=8_000_000_000, bytes_accessed=12_000_000, transcendentals=0),
        name="synthesis",
    )(on_grid, in_hbm(field), in_hbm(table), in_hbm(gain), in_hbm(up), in_hbm(bias), in_hbm(down))


def mixing_matrix(weight):
    real_weight = weight[:, :, :C]
    imag_weight = weight[:, :, C:]
    bottom_half = jnp.concatenate([-imag_weight, real_weight], axis=2)
    return jnp.concatenate([weight, bottom_half], axis=1)


def to_next(value):
    count = lax.axis_size("section")
    return lax.ppermute(value, "section", [(i, (i + 1) % count) for i in range(count)])


def to_mirrored(value):
    count = lax.axis_size("sp")
    return lax.ppermute(value, "sp", [(d, count - 1 - d) for d in range(count)])


def to_next_mirrored(value):
    sections, count = lax.axis_size("section"), lax.axis_size("sp")
    pairs = [
        (s * count + d, (s + 1) % sections * count + count - 1 - d)
        for s in range(sections)
        for d in range(count)
    ]
    return lax.ppermute(value, ("section", "sp"), pairs)


def exchange(value):
    return lax.all_to_all(value, "sp", split_axis=0, concat_axis=0)


def legendre_inputs(rank):
    pair = rank * PAIRS + jnp.minimum(jnp.arange(8, dtype=jnp.int32), PAIRS - 1)
    orders = jnp.stack([pair_low(pair), pair_high(pair)]).astype(F32)
    lane = jnp.arange(LANES, dtype=jnp.int32)
    low = (lane // ROWS) % 2 == 0
    cycle = lane // (2 * ROWS) * ROWS + lane % ROWS
    colatitude = math.pi * (cycle.astype(F32) + 0.5) / NLAT
    steps_all = jnp.arange(1, LMAX + 1, dtype=F32)
    factors = jnp.log((2.0 * steps_all - 1.0) / (2.0 * steps_all))
    below = (steps_all <= orders[:, :, None]).astype(F32)
    partial_log = jnp.sum(below * factors, axis=2)
    start = 0.5 * jnp.log((2.0 * orders + 1.0) / (4.0 * math.pi)) + 0.5 * partial_log
    order_lanes = jnp.where(low, orders[0][:, None], orders[1][:, None])
    start = jnp.where(low, start[0][:, None], start[1][:, None])
    start = (start + order_lanes * jnp.log(jnp.sin(colatitude))) * (1.0 / math.log(2.0))
    return (
        jnp.broadcast_to(orders[:, :, None], (2, 8, 128)),
        jnp.broadcast_to(jnp.cos(colatitude), (8, LANES)),
        jnp.broadcast_to(low.astype(F32), (8, LANES)),
        start,
    )


def block(field_in, spectral_gain, spectral_weight, mixer_gain, up_weight, up_bias, down_weight):
    field = field_in[0]
    rank = lax.axis_index("sp")
    weight = spectral_weight[0]
    early_weight = to_next_mirrored(weight[PAIRS : PAIRS + 3])
    spectral = analysis(rank.reshape(1), field, spectral_gain)
    rank_after, weight, _ = lax.optimization_barrier((rank, weight, spectral))
    by_order = exchange(spectral.reshape(SP, BLOCK_M, K2))
    own_weight = to_next(weight[:PAIRS])
    late_weight = to_next(weight[PAIRS + 3 :])
    legendre, table = legendre_table(*legendre_inputs(rank_after))
    first_choice = mixing_choice(rank_after, EARLY, PAIRS - EARLY)
    second_choice = mixing_choice(rank_after, 0, EARLY)

    by_order, first_choice, second_choice = lax.optimization_barrier(
        (by_order, first_choice, second_choice)
    )
    by_order = by_order.reshape(SP, PAIRS, 2 * ROWS, K2)
    first, first_diag = forward(legendre, by_order, EARLY, PAIRS - EARLY)
    first = exchange(first.reshape(SP, -1, K2))
    second, second_diag = forward(legendre, by_order, 0, EARLY)
    second, late_weight = lax.optimization_barrier((second, late_weight))
    late_weight = to_mirrored(late_weight)
    second = to_next(second)
    first = to_next(first)
    diag = to_next(first_diag + second_diag)
    second = exchange(second.reshape(SP, -1, K2))
    other_weight = jnp.concatenate([early_weight, late_weight], axis=0)
    own_matrix, other_matrix = mixing_matrix(own_weight), mixing_matrix(other_weight)
    late = PAIRS - EARLY
    mixed, diag = mixing(
        rank.reshape(1), first, first_choice, own_matrix, other_matrix, diag, late, 0
    )
    mixed, diag = mixing(
        rank.reshape(1), second, second_choice, own_matrix, other_matrix, diag,
        EARLY, BLOCK_L // PAIRS * late, mixed
    )
    back = exchange(mixed)
    grid_part = inverse(legendre, back, diag)
    on_grid = exchange(grid_part.reshape(SP, BLOCK_M, K2))
    next_field = to_next(field)
    gain_next, bias_next = to_next(mixer_gain), to_next(up_bias)
    up_next, down_next = to_next(up_weight), to_next(down_weight)
    result = synthesis(
        on_grid.reshape(MMAX * ROWS, K2),
        next_field,
        table,
        gain_next.reshape(C, 1).astype(F32),
        up_next[0].T,
        bias_next.reshape(HID, 1).astype(F32),
        down_next[0],
    )
    return result[None]


def solution(mesh):
    in_specs = (
        P("section", "sp", None, None),
        P("section", None),
        P("section", "sp", None, None),
        P("section", None),
        P("section", None, None),
        P("section", None),
        P("section", None, None),
    )
    out_specs = P("section", "sp", None, None)
    return jax.shard_map(block, mesh=mesh, in_specs=in_specs, out_specs=out_specs, check_vma=False)
```

```python
import functools
import math

import jax
import jax.numpy as jnp
from jax import lax
from jax.experimental import pallas as pl
from jax.experimental.pallas import tpu as pltpu
from jax.sharding import PartitionSpec as P


C = 192
HID = 384
NLAT = 384
NLON = 768
LMAX = 384
MMAX = 384
SP = 32
ROWS = NLAT // SP
PAIRS = LMAX // SP // 2
K2 = 2 * C
BLOCK_M = 2 * PAIRS * ROWS
BLOCK_L = 2 * PAIRS * PAIRS
EARLY = 2
SWAPPED = 4
T_ROWS = LMAX
T_PAD = T_ROWS + 8
LANES = 2 * NLAT

EPSILON = 1e-05
SCALE_LOG2 = 64.0
DOWN = 2.0**-64
LIMIT = 2.0**32

F32 = jnp.float32
BF16 = jnp.bfloat16


def pair_low(pair):
    degree = pair + pair // PAIRS * PAIRS
    return jnp.minimum(degree, LMAX - 1 - degree)


def pair_high(pair):
    degree = pair + pair // PAIRS * PAIRS
    return jnp.maximum(degree, LMAX - 1 - degree)


def params(mebibytes):
    return pltpu.CompilerParams(vmem_limit_bytes=mebibytes * 1024 * 1024)


def in_hbm(value):
    return pltpu.with_memory_space_constraint(value, pltpu.HBM)


IN_VMEM = pl.BlockSpec(memory_space=pltpu.VMEM)


def whole(shape):
    return pl.BlockSpec(shape, lambda *_: (0,) * len(shape))


def norm_rows(values, gain):
    average = jnp.mean(values, axis=0, keepdims=True)
    centred = values - average
    variance = jnp.mean(centred * centred, axis=0, keepdims=True)
    return centred * lax.rsqrt(variance + EPSILON) * gain


def remainder(values, by):
    return values - by * jnp.floor(values * (1.0 / by))


def fill_fourier_table(table_ref, scale):
    row = lax.broadcasted_iota(jnp.int32, (MMAX, 128), 0)
    pair = lax.shift_right_logical(row, 1)
    order = jnp.where(lax.bitwise_and(row, 1) == 0, pair_low(pair), pair_high(pair)).astype(F32)
    lane = lax.broadcasted_iota(jnp.int32, (MMAX, 128), 1).astype(F32)
    angle = remainder(order * lane, float(NLON)) * (2.0 * math.pi / NLON)
    factor = jnp.where(order == 0.0, 1.0, scale)
    cosine, sine = jnp.cos(angle) * factor, jnp.sin(angle) * factor
    sixth = jnp.floor(remainder(order, 6.0) + 0.5)
    half = jnp.where((sixth == 1.0) | (sixth == 5.0), 0.5, -0.5)
    turn_cos = jnp.where(sixth == 0.0, 1.0, jnp.where(sixth == 3.0, -1.0, half))
    root = math.sqrt(0.75)
    turn_sin = jnp.where((sixth == 0.0) | (sixth == 3.0), 0.0, jnp.where(sixth < 3.0, root, -root))
    for part in range(NLON // 128):
        lanes = slice(128 * part, 128 * part + 128)
        table_ref[0:MMAX, lanes] = cosine.astype(BF16)
        table_ref[MMAX : 2 * MMAX, lanes] = (-sine).astype(BF16)
        cosine, sine = cosine * turn_cos - sine * turn_sin, sine * turn_cos + cosine * turn_sin


def cycle_weights(rank):
    cycle = lax.broadcasted_iota(jnp.int32, (16, 256), 0) + rank * ROWS
    term = (lax.broadcasted_iota(jnp.int32, (16, 256), 1) + 1).astype(F32)
    turns = remainder(term * (2 * cycle + 1).astype(F32), 2.0 * NLAT)
    parts = jnp.cos(turns * (math.pi / NLAT)) / (4.0 * term * term - 1.0)
    series = jnp.sum(jnp.where(term <= NLAT // 2, parts, 0.0), axis=1, keepdims=True)
    return 2.0 / NLAT * (1.0 - 2.0 * series) * (2.0 * math.pi / NLON)


def analysis_kernel(
    rank_ref, field_ref, gain_ref, out_ref, table_ref, weight_ref, column_ref, normed_ref, acc_ref
):
    step = pl.program_id(0)

    @pl.when(step == 0)
    def _():
        for half in range(2):
            normed_ref[half, 0:64] = jnp.zeros((64, NLON), BF16)
            normed_ref[half, 256:320] = jnp.zeros((64, NLON), BF16)
        fill_fourier_table(table_ref, 1.0)
        weight_ref[...] = jnp.broadcast_to(cycle_weights(rank_ref[0]), (16, 128))
        same = lax.broadcasted_iota(jnp.int32, (C, C), 0) == lax.broadcasted_iota(jnp.int32, (C, C), 1)
        column = jnp.sum(jnp.where(same, gain_ref[...].astype(F32), 0.0), axis=1, keepdims=True)
        column_ref[...] = jnp.broadcast_to(column, (C, 128))

    @pl.when(step < ROWS // 2)
    def _():
        dims = (((1,), (1,)), ((), ()))
        gain = jnp.concatenate([column_ref[...]] * (NLON // 128), axis=1)
        for half in range(2):
            normed_ref[half, 64:256] = norm_rows(field_ref[half].astype(F32), gain).astype(BF16)
        for half in range(2):
            cycle = 2 * step + half
            weight = weight_ref[pl.ds(cycle, 1), :]
            rows = pl.ds(cycle, MMAX, stride=ROWS)
            real = lax.dot_general(
                table_ref[0:MMAX], normed_ref[half, 64:320], dims, preferred_element_type=F32
            )
            imag = lax.dot_general(
                table_ref[MMAX : 2 * MMAX], normed_ref[half, 0:256], dims, preferred_element_type=F32
            )
            acc_ref[0, rows, :] = real[:, 0:128] * weight
            acc_ref[1, rows, :] = (real[:, 128:256] + imag[:, 0:128]) * weight
            acc_ref[2, rows, :] = imag[:, 128:256] * weight

    @pl.when(step >= ROWS // 2)
    def _():
        base = (step - ROWS // 2) * (MMAX * ROWS // 6)

        @pl.loop(0, MMAX * ROWS // 6 // 128)
        def _(piece):
            into = pl.ds(pl.multiple_of(piece * 128, 128), 128)
            rows = pl.ds(pl.multiple_of(base + piece * 128, 128), 128)
            for part in range(3):
                out_ref[into, 128 * part : 128 * part + 128] = acc_ref[part, rows, :].astype(BF16)


def analysis(rank, field, gain):
    steps = ROWS // 2
    return pl.pallas_call(
        analysis_kernel,
        grid=(steps + 6,),
        in_specs=[
            pl.BlockSpec(memory_space=pltpu.SMEM),
            pl.BlockSpec((2, C, NLON), lambda j: (jnp.minimum(j, steps - 1), 0, 0)),
            whole((1, C)),
        ],
        out_specs=pl.BlockSpec((MMAX * ROWS // 6, K2), lambda j: (jnp.maximum(j - steps, 0), 0)),
        out_shape=pltpu.HBM((MMAX * ROWS, K2), BF16),
        scratch_shapes=[
            pltpu.VMEM((2 * MMAX, NLON), BF16),
            pltpu.VMEM((16, 128), F32),
            pltpu.VMEM((C, 128), F32),
            pltpu.VMEM((2, 320, NLON), BF16),
            pltpu.VMEM((3, MMAX * ROWS, 128), F32),
        ],
        compiler_params=params(28),
        cost_estimate=pl.CostEstimate(flops=3_600_000_000, bytes_accessed=9_000_000, transcendentals=0),
        name="analysis",
    )(rank, in_hbm(field), gain)


def legendre_kernel(orders_ref, cosine_ref, low_ref, start_ref, out_ref, fourier_ref, acc_ref, diag_ref):
    step = pl.program_id(0)

    @pl.when(step == 0)
    def _():
        fill_fourier_table(fourier_ref, 2.0)
        order = [orders_ref[0], orders_ref[1]]
        order_sq = [order[0] * order[0], order[1] * order[1]]
        cosine = cosine_ref[...]
        is_low = low_ref[...] > 0.5
        start = start_ref[...]
        start_level = jnp.floor(start * (1.0 / SCALE_LOG2) + 0.5)
        start_lead = jnp.exp2(start - SCALE_LOG2 * start_level)

        def spread(pair):
            return jnp.where(
                is_low,
                jnp.concatenate([pair[0]] * (LANES // 128), axis=1),
                jnp.concatenate([pair[1]] * (LANES // 128), axis=1),
            )

        order_lanes = spread(order)

        def advance(degree_index, state):
            lead, lag, level = state
            degree = degree_index.astype(F32)
            degree_sq = degree * degree
            degree_norm = jnp.maximum(4.0 * degree_sq - 1.0, 0.0)
            before_sq = (degree - 1.0) * (degree - 1.0)
            before_norm = jnp.maximum(4.0 * before_sq - 1.0, 1.0)
            leading, trailing = [], []
            for one_sq in order_sq:
                lead_coeff = jnp.sqrt(degree_norm / jnp.maximum(degree_sq - one_sq, 1.0))
                leading.append(lead_coeff)
                trailing.append(lead_coeff * jnp.sqrt(jnp.maximum(before_sq - one_sq, 0.0) / before_norm))
            following = spread(leading) * cosine * lead - spread(trailing) * lag
            first = order_lanes == degree
            lag = jnp.where(first, 0.0, lead)
            lead = jnp.where(first, start_lead, following)
            level = jnp.where(first, start_level, level)
            large = jnp.abs(lead) > LIMIT
            lead = jnp.where(large, lead * DOWN, lead)
            lag = jnp.where(large, lag * DOWN, lag)
            level = jnp.where(large, level + 1.0, level)
            value = lead * jnp.where(level > -0.5, 1.0, DOWN)
            value = value * jnp.where(level > -1.5, 1.0, jnp.where(level > -2.5, DOWN, 0.0))
            return (lead, lag, level), value, first

        def position(degree_index):
            mirrored = lax.rem(degree_index, 2 * PAIRS) >= PAIRS
            degree = jnp.where(mirrored, LMAX - 1 - degree_index, degree_index)
            pair = degree - degree // (2 * PAIRS) * PAIRS
            return pl.multiple_of(pair * 16, 16)

        def lower(degree_index, state):
            state, value, _ = advance(degree_index, state)
            rows = pl.ds(position(degree_index) + 8, 8)
            low = jnp.where(is_low, value, 0.0)
            for part in range(LANES // 128):
                acc_ref[part, rows, :] = low[:, 128 * part : 128 * part + 128]
            return state

        def upper(degree_index, state):
            state, value, first = advance(degree_index, state)
            base = position(degree_index)
            low = jnp.where(is_low, value, 0.0)
            high = jnp.where(is_low, 0.0, value)
            added = jnp.where(first, 0.0, high)
            for part in range(LANES // 128):
                lanes = slice(128 * part, 128 * part + 128)
                acc_ref[part, pl.ds(base, 8), :] = low[:, lanes]
                acc_ref[part, pl.ds(base + 8, 8), :] += added[:, lanes]
            diag_ref[...] += jnp.where(first, high, 0.0)
            return state

        diag_ref[...] = jnp.zeros_like(diag_ref)
        zero = jnp.zeros((8, LANES), F32)
        state = lax.fori_loop(0, LMAX // 2, lower, (zero, zero, zero))
        lax.fori_loop(LMAX // 2, LMAX, upper, state)

    for part in range(LANES // 128):
        rows = acc_ref[part, pl.ds(step, T_ROWS, stride=8), :]
        out_ref[0:T_ROWS, 128 * part : 128 * part + 128] = rows.astype(BF16)
    row = lax.broadcasted_iota(jnp.int32, (8, LANES), 0)
    out_ref[T_ROWS:T_PAD] = jnp.where(row == 0, diag_ref[pl.ds(step, 1), :], 0.0).astype(BF16)


def legendre_table(orders, cosine, low, start):
    return pl.pallas_call(
        legendre_kernel,
        grid=(PAIRS,),
        in_specs=[whole((2, 8, 128)), whole((8, LANES)), whole((8, LANES)), whole((8, LANES))],
        out_specs=[
            pl.BlockSpec((None, T_PAD, LANES), lambda i: (i, 0, 0)),
            whole((2 * MMAX, NLON)),
        ],
        out_shape=[pltpu.HBM((PAIRS, T_PAD, LANES), BF16), pltpu.HBM((2 * MMAX, NLON), BF16)],
        scratch_shapes=[pltpu.VMEM((LANES // 128, T_ROWS * 8, 128), F32), pltpu.VMEM((8, LANES), F32)],
        compiler_params=params(22),
        cost_estimate=pl.CostEstimate(flops=10_000_000_000, bytes_accessed=4_000_000, transcendentals=0),
        name="legendre_table",
    )(orders, cosine, low, start)


def forward_kernel(first, count, table_ref, spectral_ref, out_ref, diag_ref, acc_ref):
    step = pl.program_id(0)
    values = spectral_ref[:, first + step].reshape(LANES, K2)
    result = jnp.dot(table_ref[...], values, preferred_element_type=F32)
    for part in range(3):
        acc_ref[part, pl.ds(step, T_ROWS, stride=count), :] = result[0:T_ROWS, 128 * part : 128 * part + 128]
    row = lax.broadcasted_iota(jnp.int32, (8, K2), 0)

    @pl.when(step == 0)
    def _():
        diag_ref[...] = jnp.zeros_like(diag_ref)

    diag_ref[...] = jnp.where(row == first + step, result[T_ROWS : T_ROWS + 1], diag_ref[...])

    @pl.when(step == count - 1)
    def _():
        @pl.loop(0, T_ROWS * count // 256)
        def _(piece):
            rows = pl.ds(pl.multiple_of(piece * 256, 256), 256)
            for part in range(3):
                out_ref[rows, 128 * part : 128 * part + 128] = acc_ref[part, rows, :].astype(BF16)


def forward(table, spectral, first, count):
    return pl.pallas_call(
        functools.partial(forward_kernel, first, count),
        grid=(count,),
        in_specs=[pl.BlockSpec((None, T_PAD, LANES), lambda i: (first + i, 0, 0)), IN_VMEM],
        out_specs=[whole((T_ROWS * count, K2)), whole((8, K2))],
        out_shape=[pltpu.HBM((T_ROWS * count, K2), BF16), jax.ShapeDtypeStruct((8, K2), F32)],
        scratch_shapes=[pltpu.VMEM((3, T_ROWS * count, 128), F32)],
        compiler_params=params(14),
        cost_estimate=pl.CostEstimate(
            flops=230_000_000 * count, bytes_accessed=1_500_000 * count, transcendentals=0
        ),
        name="forward",
    )(in_hbm(table), spectral)


def mixing_choice(rank, first, count):
    block = 4 * count
    step = jnp.arange(PAIRS // 2, dtype=jnp.int32)[:, None]
    index = jnp.arange(SP * block, dtype=jnp.int32)[None, :]
    within = index % block
    local = within // (2 * count)
    second = within // count % 2
    order = pair_low(index // block * PAIRS + first + within % count)
    low_degree = pair_low(rank * PAIRS + 2 * step + local)
    uses_low = jnp.logical_and(second == 1, order <= low_degree)
    uses_own = uses_low == (rank < SP // 2)
    choice = (2 * local + uses_own.astype(jnp.int32)).astype(F32)
    return jnp.broadcast_to(choice[:, :, None], (PAIRS // 2, SP * block, 128))


def mixing_kernel(count, rank_ref, coeffs_ref, choice_ref, own_ref, other_ref, diag_ref, *refs):
    out_ref, diag_out_ref = refs[-2:]
    step = pl.program_id(0)
    block = 4 * count
    values = coeffs_ref[:, pl.ds(pl.multiple_of(block * step, 8), block), :].reshape(SP * block, K2)
    choice = jnp.concatenate([choice_ref[...]] * (K2 // 128), axis=1)
    result = []
    for pair in range(2):
        own = jnp.dot(values, own_ref[2 * step + pair], preferred_element_type=F32)
        other = jnp.dot(values, other_ref[PAIRS - 1 - 2 * step - pair], preferred_element_type=F32)
        result.append(jnp.where(choice == 2.0 * pair, other, own))
    mixed = jnp.where(choice < 1.5, result[0], result[1]).astype(BF16)
    out_ref[...] = mixed.reshape(SP, block, K2)

    if len(refs) == 2:
        own_is_low = rank_ref[0] < SP // 2

        @pl.when(step == 0)
        def _():
            diag_out_ref[...] = jnp.zeros_like(diag_out_ref)

        diag = diag_ref[...].astype(BF16)
        row = lax.broadcasted_iota(jnp.int32, (8, K2), 0)
        for pair in range(2):
            own = jnp.dot(diag, own_ref[2 * step + pair], preferred_element_type=F32)
            other = jnp.dot(diag, other_ref[PAIRS - 1 - 2 * step - pair], preferred_element_type=F32)
            chosen = jnp.where(own_is_low, other, own)
            diag_out_ref[...] = jnp.where(row == 2 * step + pair, chosen, diag_out_ref[...])
    else:
        diag_out_ref[...] = diag_ref[...]


def mixing(rank, coeffs, choice, own, other, diag, count, offset, filled=None):
    block = 4 * count
    extra = [] if filled is None else [filled]
    return pl.pallas_call(
        functools.partial(mixing_kernel, count),
        grid=(PAIRS // 2,),
        in_specs=[
            pl.BlockSpec(memory_space=pltpu.SMEM),
            IN_VMEM,
            pl.BlockSpec((None, SP * block, 128), lambda g: (g, 0, 0)),
            IN_VMEM,
            IN_VMEM,
            whole((8, K2)),
        ]
        + [pl.BlockSpec(memory_space=pl.ANY) for _ in extra],
        out_specs=[pl.BlockSpec((SP, block, K2), lambda g: (0, offset // block + g, 0)), whole((8, K2))],
        out_shape=[pltpu.HBM((SP, BLOCK_L, K2), BF16), jax.ShapeDtypeStruct((8, K2), F32)],
        input_output_aliases={6: 0} if extra else {},
        compiler_params=params(14),
        cost_estimate=pl.CostEstimate(
            flops=450_000_000 * count, bytes_accessed=1_200_000 * count, transcendentals=0
        ),
        name="mixing",
    )(rank, coeffs, in_hbm(choice), own, other, diag, *extra)


def inverse_kernel(table_ref, mixed_ref, diag_ref, out_ref, early_ref, late_ref, values_ref):
    step = pl.program_id(0)
    split = BLOCK_L // PAIRS * (PAIRS - EARLY)
    rest = BLOCK_L - split

    @pl.when(step == 0)
    def _():
        @pl.loop(0, SP)
        def _(owner):
            early = pl.ds(pl.multiple_of(owner * split, 8), split)
            late = pl.ds(pl.multiple_of(owner * rest, 8), rest)
            for part in range(3):
                lanes = slice(128 * part, 128 * part + 128)
                early_ref[part, early, :] = mixed_ref[owner, 0:split, lanes].astype(F32)
                late_ref[part, late, :] = mixed_ref[owner, split:BLOCK_L, lanes].astype(F32)

    @pl.when(step < EARLY)
    def _():
        rows = pl.ds(step, T_ROWS, stride=EARLY)
        for part in range(3):
            values_ref[:, 128 * part : 128 * part + 128] = late_ref[part, rows, :].astype(BF16)

    @pl.when(step >= EARLY)
    def _():
        rows = pl.ds(step - EARLY, T_ROWS, stride=PAIRS - EARLY)
        for part in range(3):
            values_ref[:, 128 * part : 128 * part + 128] = early_ref[part, rows, :].astype(BF16)

    row = lax.broadcasted_iota(jnp.int32, (8, K2), 0)
    diag = jnp.where(row == 0, diag_ref[pl.ds(step, 1), :], 0.0).astype(BF16)
    dims = (((0,), (0,)), ((), ()))
    result = lax.dot_general(table_ref[step, 0:T_ROWS], values_ref[...], dims, preferred_element_type=F32)
    result += lax.dot_general(table_ref[step, T_ROWS:T_PAD], diag, dims, preferred_element_type=F32)
    out_ref[...] = result.astype(BF16).reshape(SP, 2 * ROWS, K2)


def inverse(table, mixed, diag):
    return pl.pallas_call(
        inverse_kernel,
        grid=(PAIRS,),
        in_specs=[IN_VMEM, IN_VMEM, whole((8, K2))],
        out_specs=pl.BlockSpec((SP, None, 2 * ROWS, K2), lambda i: (0, i, 0, 0)),
        out_shape=pltpu.HBM((SP, PAIRS, 2 * ROWS, K2), BF16),
        scratch_shapes=[
            pltpu.VMEM((3, T_ROWS * (PAIRS - EARLY), 128), F32),
            pltpu.VMEM((3, T_ROWS * EARLY, 128), F32),
            pltpu.VMEM((T_ROWS, K2), BF16),
        ],
        compiler_params=params(16),
        cost_estimate=pl.CostEstimate(flops=1_400_000_000, bytes_accessed=9_000_000, transcendentals=0),
        name="inverse",
    )(table, mixed, diag)


def synthesis_kernel(
    grid_ref, field_ref, table_ref, gain_ref, up_ref, bias_ref, down_ref, out_ref, acc_ref
):
    step = pl.program_id(0)

    @pl.when(step == 0)
    def _():
        @pl.loop(0, MMAX * ROWS // 256)
        def _(piece):
            rows = pl.ds(pl.multiple_of(piece * 256, 256), 256)
            for part in range(3):
                acc_ref[part, rows, :] = grid_ref[rows, 128 * part : 128 * part + 128].astype(F32)

    residuals = []
    for half in range(2):
        rows = pl.ds(2 * step + half, MMAX, stride=ROWS)
        values = jnp.concatenate([acc_ref[part, rows, :] for part in range(3)], axis=1)
        turned = values.T.astype(BF16)
        residual = field_ref[half].astype(F32)
        residual += jnp.dot(turned[0:C], table_ref[0:MMAX], preferred_element_type=F32)
        residual += jnp.dot(turned[C:K2], table_ref[MMAX : 2 * MMAX], preferred_element_type=F32)
        residuals.append(residual)
    for half in range(2):
        hidden_in = norm_rows(residuals[half], gain_ref[...]).astype(BF16)
        hidden = jnp.dot(up_ref[...], hidden_in, preferred_element_type=F32) + bias_ref[...]
        hidden = hidden * (1.0 + lax.erf(hidden * math.sqrt(0.5))) * 0.5
        branch = jnp.dot(down_ref[...], hidden.astype(BF16), preferred_element_type=F32)
        out_ref[half] = (residuals[half] + branch).astype(BF16)


def synthesis(on_grid, field, table, gain, up, bias, down):
    cycle = pl.BlockSpec((2, C, NLON), lambda j: (j, 0, 0))
    return pl.pallas_call(
        synthesis_kernel,
        grid=(ROWS // 2,),
        in_specs=[
            IN_VMEM,
            cycle,
            whole((2 * MMAX, NLON)),
            whole((C, 1)),
            whole((HID, C)),
            whole((HID, 1)),
            whole((C, HID)),
        ],
        out_specs=cycle,
        out_shape=jax.ShapeDtypeStruct((ROWS, C, NLON), BF16),
        scratch_shapes=[pltpu.VMEM((3, MMAX * ROWS, 128), F32)],
        compiler_params=params(32),
        cost_estimate=pl.CostEstimate(flops=8_000_000_000, bytes_accessed=12_000_000, transcendentals=0),
        name="synthesis",
    )(on_grid, in_hbm(field), in_hbm(table), in_hbm(gain), in_hbm(up), in_hbm(bias), in_hbm(down))


def mixing_matrix(weight):
    real_weight = weight[:, :, :C]
    imag_weight = weight[:, :, C:]
    bottom_half = jnp.concatenate([-imag_weight, real_weight], axis=2)
    return jnp.concatenate([weight, bottom_half], axis=1)


def to_next(value):
    count = lax.axis_size("section")
    return lax.ppermute(value, "section", [(i, (i + 1) % count) for i in range(count)])


def to_mirrored(value):
    count = lax.axis_size("sp")
    return lax.ppermute(value, "sp", [(d, count - 1 - d) for d in range(count)])


def to_next_mirrored(value):
    sections, count = lax.axis_size("section"), lax.axis_size("sp")
    pairs = [
        (s * count + d, (s + 1) % sections * count + count - 1 - d)
        for s in range(sections)
        for d in range(count)
    ]
    return lax.ppermute(value, ("section", "sp"), pairs)


def exchange(value):
    return lax.all_to_all(value, "sp", split_axis=0, concat_axis=0)


def legendre_inputs(rank):
    pair = rank * PAIRS + jnp.minimum(jnp.arange(8, dtype=jnp.int32), PAIRS - 1)
    orders = jnp.stack([pair_low(pair), pair_high(pair)]).astype(F32)
    lane = jnp.arange(LANES, dtype=jnp.int32)
    low = (lane // ROWS) % 2 == 0
    cycle = lane // (2 * ROWS) * ROWS + lane % ROWS
    colatitude = math.pi * (cycle.astype(F32) + 0.5) / NLAT
    steps_all = jnp.arange(1, LMAX + 1, dtype=F32)
    factors = jnp.log((2.0 * steps_all - 1.0) / (2.0 * steps_all))
    below = (steps_all <= orders[:, :, None]).astype(F32)
    partial_log = jnp.sum(below * factors, axis=2)
    start = 0.5 * jnp.log((2.0 * orders + 1.0) / (4.0 * math.pi)) + 0.5 * partial_log
    order_lanes = jnp.where(low, orders[0][:, None], orders[1][:, None])
    start = jnp.where(low, start[0][:, None], start[1][:, None])
    start = (start + order_lanes * jnp.log(jnp.sin(colatitude))) * (1.0 / math.log(2.0))
    return (
        jnp.broadcast_to(orders[:, :, None], (2, 8, 128)),
        jnp.broadcast_to(jnp.cos(colatitude), (8, LANES)),
        jnp.broadcast_to(low.astype(F32), (8, LANES)),
        start,
    )


def block(field_in, spectral_gain, spectral_weight, mixer_gain, up_weight, up_bias, down_weight):
    field = field_in[0]
    rank = lax.axis_index("sp")
    weight = spectral_weight[0]
    early_weight = to_next_mirrored(weight[PAIRS : PAIRS + SWAPPED])
    spectral = analysis(rank.reshape(1), field, spectral_gain)
    rank_after, weight, _ = lax.optimization_barrier((rank, weight, spectral))
    by_order = exchange(spectral.reshape(SP, BLOCK_M, K2))
    own_weight = to_next(weight[:PAIRS])
    late_weight = to_next(weight[PAIRS + SWAPPED :])
    legendre, table = legendre_table(*legendre_inputs(rank_after))
    first_choice = mixing_choice(rank_after, EARLY, PAIRS - EARLY)
    second_choice = mixing_choice(rank_after, 0, EARLY)

    by_order, first_choice, second_choice = lax.optimization_barrier(
        (by_order, first_choice, second_choice)
    )
    by_order = by_order.reshape(SP, PAIRS, 2 * ROWS, K2)
    first, first_diag = forward(legendre, by_order, EARLY, PAIRS - EARLY)
    first = exchange(first.reshape(SP, -1, K2))
    second, second_diag = forward(legendre, by_order, 0, EARLY)
    second, late_weight = lax.optimization_barrier((second, late_weight))
    late_weight = to_mirrored(late_weight)
    second = to_next(second)
    first = to_next(first)
    diag = to_next(first_diag + second_diag)
    second = exchange(second.reshape(SP, -1, K2))
    other_weight = jnp.concatenate([early_weight, late_weight], axis=0)
    own_matrix, other_matrix = mixing_matrix(own_weight), mixing_matrix(other_weight)
    late = PAIRS - EARLY
    mixed, diag = mixing(
        rank.reshape(1), first, first_choice, own_matrix, other_matrix, diag, late, 0
    )
    mixed, diag = mixing(
        rank.reshape(1), second, second_choice, own_matrix, other_matrix, diag,
        EARLY, BLOCK_L // PAIRS * late, mixed
    )
    back = exchange(mixed)
    grid_part = inverse(legendre, back, diag)
    on_grid = exchange(grid_part.reshape(SP, BLOCK_M, K2))
    next_field = to_next(field)
    gain_next, bias_next = to_next(mixer_gain), to_next(up_bias)
    up_next, down_next = to_next(up_weight), to_next(down_weight)
    result = synthesis(
        on_grid.reshape(MMAX * ROWS, K2),
        next_field,
        table,
        gain_next.reshape(C, 1).astype(F32),
        up_next[0].T,
        bias_next.reshape(HID, 1).astype(F32),
        down_next[0],
    )
    return result[None]


def solution(mesh):
    in_specs = (
        P("section", "sp", None, None),
        P("section", None),
        P("section", "sp", None, None),
        P("section", None),
        P("section", None, None),
        P("section", None),
        P("section", None, None),
    )
    out_specs = P("section", "sp", None, None)
    return jax.shard_map(block, mesh=mesh, in_specs=in_specs, out_specs=out_specs, check_vma=False)
```
